32 devices in a mesh: lat: 8 (over y, x, core), lon: 4 (over z).
Axes of the slice: x: 2, y: 2, z: 4, core: 2. Of those that a mesh axis runs over, the one named last changes fastest.
Arguments:
- loadings: float32 [176, 720, 200], P('lat', 'lon'), may hold values from -60 to 60, as said below
Outputs:
- rotated: float32 [176, 720, 200], P('lat', 'lon')
- rotation: float32 [200, 200], replicated
The draws below stay inside these ranges and needn't reach their ends.
Inputs may be any that keep to these rules, and one draw needn't show every extreme that they name: Every grid point's loadings are not all zero.
All inputs are finite; a program needn't handle non-finite values.
Results may differ from the reference program's by a relative error of at most 0.00011.
Values sent between devices are 32-bit elements; how exact they have to be, the bound alone decides.
A program may use at most 64 MiB of HBM per device.

```python
import math
import jax
import jax.numpy as jnp
from jax import lax

K = 200
LAT_DEV = 22
SWEEPS = 2
NS_STEPS = 20
NLAT = 176
NLON = 720
N_LAT = 8


def draw_loadings(key, part):
    base_key = jax.random.fold_in(key, 17)
    keys = jax.random.split(base_key, 8)
    rows = jnp.arange(NLAT).astype(jnp.int32)[:, None]
    cols = jnp.arange(NLON).astype(jnp.int32)[None, :]
    region = rows * 10 // NLAT * 20 + cols * 20 // NLON
    order = jax.random.permutation(keys[0], K).astype(jnp.int32)
    primary = order[region % K]
    secondary = order[(region + 20 + rows % 3) % K]
    flips = jax.random.randint(keys[1], (NLAT, NLON, 1), 0, 2).astype(jnp.float32) * 2.0 - 1.0
    modes = jnp.arange(K).astype(jnp.int32)[None, None, :]
    noise = 0.25 * jnp.clip(jax.random.normal(keys[2], (NLAT, NLON, K), jnp.float32), -3.0, 3.0)
    strength = 2.0 + jnp.abs(jnp.clip(jax.random.normal(keys[3], (NLAT, NLON, 1), jnp.float32), -3.0, 3.0))
    row_scale = jnp.exp(jax.random.uniform(keys[5], (NLAT, NLON, 1), jnp.float32) * math.log(10.0))
    side = 0.5 * strength * jax.random.uniform(keys[4], (NLAT, NLON, 1), jnp.float32, -1.0, 1.0)
    structure = noise + jnp.where(modes == primary[:, :, None], flips * strength, 0.0)
    structure = structure + jnp.where(modes == secondary[:, :, None], side, 0.0)
    col_scale = jnp.exp(jax.random.uniform(keys[6], (1, 1, K), jnp.float32, -1.0, 0.0) * math.log(3.0))
    structure = structure * row_scale * col_scale
    gauss = jax.random.normal(keys[7], (K, K), jnp.float32)
    ortho, upper = jnp.linalg.qr(gauss)
    ortho = ortho * jnp.where(jnp.diagonal(upper) >= 0.0, 1.0, -1.0)[None, :]
    mixed = jnp.dot(structure.reshape(NLAT * NLON, K), ortho, precision=lax.Precision.HIGHEST)
    return jnp.clip(mixed.reshape(NLAT, NLON, K), -60.0, 60.0)


def setup_inputs(seed: int = 0) -> dict:
    key_list = jax.random.split(jax.random.key(seed), 2)
    loadings = draw_loadings(jax.random.fold_in(key_list[1], 71), 0)
    return dict(loadings=loadings)


def grid_weights():
    rows = jnp.arange(NLAT).astype(jnp.float32)
    degrees = -90.0 + (rows + 0.5) * (180.0 / NLAT)
    return jnp.cos(degrees * (math.pi / 180.0))

def matmul(left, right):
    return jnp.dot(left, right, precision=lax.Precision.HIGHEST)

def polar_factor(gradient):
    iterate = gradient / jnp.sqrt(jnp.sum(gradient * gradient))
    for count in range(NS_STEPS):
        iterate = 1.5 * iterate - 0.5 * matmul(iterate, matmul(iterate.T, iterate))
    return iterate

def reference(loadings):
    row_norm = jnp.sqrt(lax.optimization_barrier(jnp.sum(loadings * loadings, axis=-1, keepdims=True)) + 1e-06)
    normed = loadings / row_norm
    weights = grid_weights()
    total = jnp.sum(weights) * NLON
    bands = normed.reshape(N_LAT, LAT_DEV * NLON, K)
    band_weights = jnp.repeat(weights.reshape(N_LAT, LAT_DEV), NLON, axis=1).reshape(N_LAT, LAT_DEV * NLON, 1)
    rotation = jnp.eye(K, dtype=jnp.float32)
    for sweep_index in range(SWEEPS):

        def colsq_band(carry, pair):
            block, block_weights = pair
            spun = matmul(block, rotation)
            return (carry + lax.optimization_barrier(jnp.sum(block_weights * spun * spun, axis=0)), None)
        colsq, unused = lax.scan(colsq_band, jnp.zeros((K,), jnp.float32), (bands, band_weights))

        def gradient_band(carry, pair):
            block, block_weights = pair
            spun = matmul(block, rotation)
            term = block_weights * (spun * spun * spun - spun * (colsq / total)[None, :])
            return (carry + matmul(block.T, term), None)
        gradient, unused = lax.scan(gradient_band, jnp.zeros((K, K), jnp.float32), (bands, band_weights))
        rotation = polar_factor(gradient)
    flat = normed.reshape(NLAT * NLON, K)
    rotated = matmul(flat, rotation).reshape(NLAT, NLON, K) * row_norm
    return (rotated, rotation)
```

```python
import functools
import math

import jax
import jax.numpy as jnp
import numpy as np
from jax import lax
from jax.experimental import pallas as pl
from jax.experimental.pallas import tpu as pltpu
from jax.sharding import PartitionSpec as P

SWEEPS = 2
NS_STEPS = 20
SUB = 8
LANES = 256
CORES = 2
MESH = pl.DeviceIdType.MESH
NN = (((1,), (0,)), ((), ()))
NT = (((1,), (1,)), ((), ()))


def split(value):
    high = value.astype(jnp.bfloat16)
    low = (value - high.astype(jnp.float32)).astype(jnp.bfloat16)
    return high, low


def mm(left, right, dims=NN):
    return lax.dot_general(left, right, dims, preferred_element_type=jnp.float32)


def mm3(left, right, dims=NN):
    lh, ll = left
    rh, rl = right
    return mm(lh, rh, dims) + (mm(lh, rl, dims) + mm(ll, rh, dims))


def polar(gradient):
    squares = jnp.sum(gradient * gradient, axis=0, keepdims=True)
    norm = jnp.sqrt(jnp.sum(squares, axis=1, keepdims=True))

    def step(_, x):
        parts = split(x)
        inner = mm3(parts, parts, NT)
        return 1.5 * x - 0.5 * mm3(split(inner), parts)

    return lax.fori_loop(0, NS_STEPS, step, gradient / norm, unroll=4)


class Mesh:
    def __init__(self, n_lat, n_lon):
        self.n_lon, self.n = n_lon, n_lat * n_lon
        self.chips = self.n // CORES
        lat, lon = lax.axis_index("lat"), lax.axis_index("lon")
        self.lat = lat
        self.me = lat * n_lon + lon
        self.core = lax.rem(lat, CORES)
        self.other = 1 - self.core
        self.chip = (lat // CORES) * n_lon + lon

    def device(self, index):
        return index // self.n_lon, lax.rem(index, self.n_lon)

    def seat(self, chip, core):
        return (chip // self.n_lon) * CORES + core, lax.rem(chip, self.n_lon)


def remote(source, target, sems, phase, device):
    return pltpu.make_async_remote_copy(
        src_ref=source,
        dst_ref=target,
        send_sem=sems.at[phase, 0],
        recv_sem=sems.at[phase, 1],
        device_id=device,
        device_id_type=MESH,
    )


class Reduce:
    def __init__(self, mesh, owners, bufs, sems):
        self.mesh, self.owners = mesh, owners
        self.part, self.peer, self.chip_sum, self.got, self.full, self.rows = bufs
        self.sems = sems

    def spread(self, value):
        mesh = self.mesh
        self.rows[mesh.me, :, : value.shape[1]] = value
        for shift in range(1, mesh.n):
            row = self.rows.at[mesh.me]
            remote(row, row, self.sems, 0, mesh.device(lax.rem(mesh.me + shift, mesh.n))).start()

    def others(self):
        rest = self.rows.at[pl.ds(0, self.mesh.n - 1)]
        return remote(rest, rest, self.sems, 0, self.mesh.device(self.mesh.me))

    def total(self, width):
        self.others().wait_recv()
        acc = self.rows[0]
        for source in range(1, self.mesh.n):
            acc = acc + self.rows[source]
        return acc[:, :width]

    def swap(self):
        mesh = self.mesh
        return remote(self.part.at[mesh.other], self.peer, self.sems, 1,
                      mesh.seat(mesh.chip, mesh.other))

    def scatter(self, owner):
        mesh = self.mesh
        return remote(self.chip_sum.at[owner], self.got.at[mesh.chip], self.sems, 2,
                      mesh.seat(owner, mesh.core))

    def gather(self, chip, blocks):
        mesh = self.mesh
        block = self.full.at[mesh.core, blocks]
        return remote(block, block, self.sems, 3, mesh.seat(chip, mesh.core))

    def share(self):
        mesh = self.mesh
        half = self.full.at[mesh.core]
        return remote(half, half, self.sems, 4, mesh.seat(mesh.chip, mesh.other))

    def reduce(self):
        mesh, owners = self.mesh, self.owners
        chip, chips = mesh.chip, mesh.chips
        self.swap().start()
        self.swap().wait_recv()
        self.chip_sum[...] = self.part[mesh.core] + self.peer[...]
        for shift in range(1, chips):
            owner = lax.rem(chip + shift, chips)

            @pl.when(owner < owners)
            def _():
                self.scatter(owner).start()

        @pl.when(chip < owners)
        def _():
            rest = self.got.at[pl.ds(0, chips - 1)]
            remote(rest, rest, self.sems, 2, mesh.seat(chip, mesh.core)).wait_recv()
            acc = self.chip_sum[chip]
            for shift in range(1, chips):
                acc = acc + self.got[lax.rem(chip + shift, chips)]
            self.full[mesh.core, chip] = acc
            for shift in range(1, chips):
                self.gather(lax.rem(chip + shift, chips), chip).start()
            self.gather(chip, pl.ds(0, owners - 1)).wait_recv()

        @pl.when(chip >= owners)
        def _():
            self.gather(chip, pl.ds(0, owners)).wait_recv()

        self.share().start()
        self.share().wait_recv()

    def finish(self):
        mesh, owners = self.mesh, self.owners
        chip, chips = mesh.chip, mesh.chips
        self.others().wait_send()
        self.swap().wait_send()
        self.share().wait_send()

        @pl.when(chip < owners)
        def _():
            rest = self.got.at[pl.ds(0, owners - 1)]
            remote(rest, rest, self.sems, 2, mesh.seat(chip, mesh.core)).wait_send()
            rest = self.got.at[pl.ds(0, chips - 1)]
            remote(rest, rest, self.sems, 3, mesh.seat(chip, mesh.core)).wait_send()

        @pl.when(chip >= owners)
        def _():
            rest = self.got.at[pl.ds(0, owners)]
            remote(rest, rest, self.sems, 2, mesh.seat(chip, mesh.core)).wait_send()


def halves(value, owners):
    modes = value.shape[0]
    rows = owners * SUB
    return value[:rows].reshape(owners, SUB, modes), value[rows:].reshape(-1, SUB, modes)


def store_halves(part, value, owners):
    modes = value.shape[1]
    low, high = halves(value, owners)
    part[0, :, :, :modes] = low
    part[1, : high.shape[0], :, :modes] = high


def whole(full, modes):
    blocks = [full[0, :, :, :modes].reshape(-1, modes), full[1, :, :, :modes].reshape(-1, modes)]
    return jnp.concatenate(blocks, axis=0)[:modes]


def kernel(n_lat, n_lon, total, weights, loadings, out, held, yh, yl, th, tl, gram, cubic,
           part1, peer1, sum1, got1, full1, rows1, part2, peer2, sum2, got2, full2, rows2,
           sems1, sems2, loads):
    lat_rows, lon_cols, modes = held.shape
    mesh = Mesh(n_lat, n_lon)
    n, me, lat = mesh.n, mesh.me, mesh.lat
    owners = part1.shape[1]
    unroll = next(k for k in (11, 4, 3, 2, 1) if lat_rows % k == 0)
    reduce1 = Reduce(mesh, owners, (part1, peer1, sum1, got1, full1, rows1), sems1)
    reduce2 = Reduce(mesh, owners, (part2, peer2, sum2, got2, full2, rows2), sems2)

    def load(j):
        return pltpu.make_async_copy(loadings.at[j], held.at[j], loads.at[j])

    for j in range(lat_rows):
        load(j).start()
    barrier = pltpu.get_barrier_semaphore()
    for shift in range(1, n):
        peer = lax.rem(me + shift, n)
        pl.semaphore_signal(barrier, inc=1, device_id=mesh.device(peer), device_id_type=MESH)

    def rows_of(body, init):
        def step(i, carry):
            for k in range(unroll):
                carry = body(i * unroll + k, carry)
            return carry

        return lax.fori_loop(0, lat_rows // unroll, step, init)

    def normalise(j, colsq):
        load(j).wait()
        x = held[j]
        root = weights[1, lat * lat_rows + j]
        y = x * (root / jnp.sqrt(jnp.sum(x * x, axis=1, keepdims=True) + 1e-06))
        held[j] = y
        yh[j], yl[j] = split(y)
        return colsq + jnp.sum(y * y, axis=0, keepdims=True)

    none = jnp.zeros((1, modes), jnp.float32)
    colsq = rows_of(normalise, none)
    gram[...] = jnp.zeros_like(gram)
    cubic[...] = jnp.zeros_like(cubic)
    part1[...] = jnp.zeros_like(part1)
    part2[...] = jnp.zeros_like(part2)
    pl.semaphore_wait(barrier, n - 1)
    reduce1.spread(colsq)

    def first(i, carry):
        grams, cubics = [], []
        for k in range(unroll):
            j = i * unroll + k
            y = held[j]
            t_parts = split(y.T)
            th[j], tl[j] = t_parts
            inverse = weights[2, lat * lat_rows + j]
            grams.append(mm3(t_parts, (yh[j], yl[j])))
            cubics.append(mm3(t_parts, split(y * y * y * inverse)))
        gram[...] += sum(grams[1:], grams[0])
        cubic[...] += sum(cubics[1:], cubics[0])
        return carry

    lax.fori_loop(0, lat_rows // unroll, first, 0)
    colsq = reduce1.total(modes)
    store_halves(part1, cubic[...] - gram[...] * (colsq / total), owners)
    reduce1.reduce()
    cubic[...] = jnp.zeros_like(cubic)
    rotation = polar(whole(full1, modes))
    r_parts = split(rotation)

    def spin(j, colsq):
        spun = mm3((yh[j], yl[j]), r_parts)
        held[j] = spun
        return colsq + jnp.sum(spun * spun, axis=0, keepdims=True)

    reduce2.spread(rows_of(spin, none))

    def second(i, carry):
        cubics = []
        for k in range(unroll):
            j = i * unroll + k
            spun = held[j]
            inverse = weights[2, lat * lat_rows + j]
            cubics.append(mm3((th[j], tl[j]), split(spun * spun * spun * inverse)))
        cubic[...] += sum(cubics[1:], cubics[0])
        return carry

    lax.fori_loop(0, lat_rows // unroll, second, 0)
    turned = mm3(split(gram[...]), r_parts)
    colsq = reduce2.total(modes)
    store_halves(part2, cubic[...] - turned * (colsq / total), owners)
    reduce2.reduce()
    out[...] = whole(full2, modes)
    reduce1.finish()
    reduce2.finish()


def turn(gradient, loadings, rotated, rotation, held, result, load, stores):
    lat_rows = held.shape[0]
    fetch = pltpu.make_async_copy(loadings, held, load)
    fetch.start()
    result[...] = polar(gradient[...])
    save = pltpu.make_async_copy(result, rotation, stores.at[0])
    save.start()
    r_parts = split(result[...])
    fetch.wait()
    unroll = next(k for k in (2, 1) if lat_rows % k == 0)

    def step(i, carry):
        for k in range(unroll):
            j = i * unroll + k
            held[j] = mm3(split(held[j]), r_parts)
            pltpu.make_async_copy(held.at[j], rotated.at[j], stores.at[1]).start()
        return carry

    lax.fori_loop(0, lat_rows // unroll, step, 0)
    save.wait()
    pltpu.make_async_copy(held, rotated, stores.at[1]).wait()


def latitude_weight(lat_total):
    rows = np.arange(lat_total, dtype=np.float32)
    degrees = np.float32(-90.0) + (rows + np.float32(0.5)) * np.float32(180.0 / lat_total)
    return np.cos(degrees * np.float32(math.pi / 180.0)).astype(np.float32)


def shards(n_lat, n_lon, loadings):
    lat_rows, lon_cols, modes = loadings.shape
    n = n_lat * n_lon
    owners = -(-modes // (CORES * SUB))
    assert n_lat % CORES == 0 and modes % SUB == 0 and modes <= LANES
    assert 1 < owners <= n // CORES
    weights = latitude_weight(lat_rows * n_lat)
    total = float(np.sum(weights, dtype=np.float32) * np.float32(lon_cols * n_lon))
    table = jnp.asarray(np.stack([weights, np.sqrt(weights), 1.0 / weights]).astype(np.float32))
    f32, bf16 = jnp.float32, jnp.bfloat16

    bufs = [
        pltpu.VMEM((CORES, owners, SUB, LANES), f32),
        pltpu.VMEM((owners, SUB, LANES), f32),
        pltpu.VMEM((owners, SUB, LANES), f32),
        pltpu.VMEM((n // CORES, SUB, LANES), f32),
        pltpu.VMEM((CORES, owners, SUB, LANES), f32),
        pltpu.VMEM((n, 1, LANES), f32),
    ]

    gradient = pl.pallas_call(
        functools.partial(kernel, n_lat, n_lon, total),
        out_shape=jax.ShapeDtypeStruct((modes, modes), f32),
        in_specs=[
            pl.BlockSpec(memory_space=pltpu.SMEM),
            pl.BlockSpec(memory_space=pl.ANY),
        ],
        out_specs=pl.BlockSpec(memory_space=pltpu.VMEM),
        scratch_shapes=[
            pltpu.VMEM((lat_rows, lon_cols, modes), f32),
            pltpu.VMEM((lat_rows, lon_cols, modes), bf16),
            pltpu.VMEM((lat_rows, lon_cols, modes), bf16),
            pltpu.VMEM((lat_rows, modes, lon_cols), bf16),
            pltpu.VMEM((lat_rows, modes, lon_cols), bf16),
            pltpu.VMEM((modes, modes), f32),
            pltpu.VMEM((modes, modes), f32),
            *bufs,
            *bufs,
            pltpu.SemaphoreType.DMA((5, 2)),
            pltpu.SemaphoreType.DMA((5, 2)),
            pltpu.SemaphoreType.DMA((lat_rows,)),
        ],
        compiler_params=pltpu.CompilerParams(
            collective_id=0, has_side_effects=True, vmem_limit_bytes=60 * 1024 * 1024
        ),
    )(table, loadings)
    return pl.pallas_call(
        turn,
        out_shape=(
            jax.ShapeDtypeStruct(loadings.shape, f32),
            jax.ShapeDtypeStruct((modes, modes), f32),
        ),
        in_specs=[
            pl.BlockSpec(memory_space=pltpu.VMEM),
            pl.BlockSpec(memory_space=pl.ANY),
        ],
        out_specs=(
            pl.BlockSpec(memory_space=pl.ANY),
            pl.BlockSpec(memory_space=pl.ANY),
        ),
        scratch_shapes=[
            pltpu.VMEM((lat_rows, lon_cols, modes), f32),
            pltpu.VMEM((modes, modes), f32),
            pltpu.SemaphoreType.DMA,
            pltpu.SemaphoreType.DMA((2,)),
        ],
        compiler_params=pltpu.CompilerParams(vmem_limit_bytes=60 * 1024 * 1024),
    )(gradient, loadings)


def solution(mesh):
    return jax.shard_map(
        functools.partial(shards, mesh.shape["lat"], mesh.shape["lon"]),
        mesh=mesh,
        in_specs=(P("lat", "lon", None),),
        out_specs=(P("lat", "lon", None), P()),
        check_vma=False,
    )
```

```python
import functools
import math

import jax
import jax.numpy as jnp
import numpy as np
from jax import lax
from jax.experimental import pallas as pl
from jax.experimental.pallas import tpu as pltpu
from jax.sharding import PartitionSpec as P

SWEEPS = 2
NS_STEPS = 20
SUB = 8
LANES = 256
CORES = 2
DEPTH = 256
MESH = pl.DeviceIdType.MESH
NN = (((1,), (0,)), ((), ()))
NT = (((1,), (1,)), ((), ()))


def split(value):
    high = value.astype(jnp.bfloat16)
    low = (value - high.astype(jnp.float32)).astype(jnp.bfloat16)
    return high, low


def mm(left, right, dims=NN):
    return lax.dot_general(left, right, dims, preferred_element_type=jnp.float32)


def mm3(left, right, dims=NN):
    lh, ll = left
    rh, rl = right
    return mm(lh, rh, dims) + (mm(lh, rl, dims) + mm(ll, rh, dims))


def mm_rows(rows, right, dims):
    high, low = rows
    count = high.shape[0]
    both = mm(jnp.concatenate([high, low], axis=0), right[0], dims)
    return both[:count] + (both[count:] + mm(high, right[1], dims))


def polar(gradient):
    squares = jnp.sum(gradient * gradient, axis=0, keepdims=True)
    norm = jnp.sqrt(jnp.sum(squares, axis=1, keepdims=True))
    modes = gradient.shape[0]
    cut = -(-modes // (4 * SUB)) * 2 * SUB

    def step(_, rows):
        pieces = [split(x) for x in rows]
        parts = [jnp.concatenate(side, axis=0) for side in zip(*pieces)]
        inner = [mm_rows(piece, parts, NT) for piece in pieces]
        turned = [mm_rows(split(x), parts, NN) for x in inner]
        return tuple(1.5 * x - 0.5 * y for x, y in zip(rows, turned))

    start = gradient / norm
    rows = lax.fori_loop(0, NS_STEPS, step, (start[:cut], start[cut:]), unroll=4)
    return jnp.concatenate(rows, axis=0)


class Mesh:
    def __init__(self, n_lat, n_lon):
        self.n_lon, self.n = n_lon, n_lat * n_lon
        self.chips = self.n // CORES
        lat, lon = lax.axis_index("lat"), lax.axis_index("lon")
        self.lat = lat
        self.me = lat * n_lon + lon
        self.core = lax.rem(lat, CORES)
        self.other = 1 - self.core
        self.chip = (lat // CORES) * n_lon + lon

    def device(self, index):
        return index // self.n_lon, lax.rem(index, self.n_lon)

    def seat(self, chip, core):
        return (chip // self.n_lon) * CORES + core, lax.rem(chip, self.n_lon)


def remote(source, target, sems, phase, device):
    return pltpu.make_async_remote_copy(
        src_ref=source,
        dst_ref=target,
        send_sem=sems.at[phase, 0],
        recv_sem=sems.at[phase, 1],
        device_id=device,
        device_id_type=MESH,
    )


class Reduce:
    def __init__(self, mesh, owners, modes, bufs, sems):
        self.mesh, self.owners = mesh, owners
        self.part, self.peer, self.chip_sum, self.got, self.full, self.rows = bufs
        self.modes = modes
        self.sems = sems

    def spread(self, value):
        mesh = self.mesh
        self.rows[mesh.me, :, : value.shape[1]] = value
        for shift in range(1, mesh.n):
            row = self.rows.at[mesh.me]
            remote(row, row, self.sems, 0, mesh.device(lax.rem(mesh.me + shift, mesh.n))).start()

    def others(self):
        rest = self.rows.at[pl.ds(0, self.mesh.n - 1)]
        return remote(rest, rest, self.sems, 0, self.mesh.device(self.mesh.me))

    def total(self):
        self.others().wait_recv()
        acc = self.rows[0]
        for source in range(1, self.mesh.n):
            acc = acc + self.rows[source]
        return acc

    def swap(self, term):
        mesh = self.mesh
        return remote(self.part.at[term, mesh.other], self.peer.at[term], self.sems, 4 + term,
                      mesh.seat(mesh.chip, mesh.other))

    def send(self, term, value):
        rows = self.owners * SUB
        modes = self.modes
        low, high = value[:rows], value[rows:]
        self.part[term, 0, :, :, :modes] = low.reshape(-1, SUB, modes)
        self.part[term, 1, : high.shape[0] // SUB, :, :modes] = high.reshape(-1, SUB, modes)
        self.swap(term).start()

    def joined(self, term):
        self.swap(term).wait_recv()
        return self.part[term, self.mesh.core] + self.peer[term]

    def scatter(self, owner):
        mesh = self.mesh
        return remote(self.chip_sum.at[owner], self.got.at[mesh.chip], self.sems, 2,
                      mesh.seat(owner, mesh.core))

    def gather(self, chip, blocks):
        mesh = self.mesh
        block = self.full.at[mesh.core, blocks]
        return remote(block, block, self.sems, 3, mesh.seat(chip, mesh.core))

    def share(self):
        mesh = self.mesh
        half = self.full.at[mesh.core]
        return remote(half, half, self.sems, 1, mesh.seat(mesh.chip, mesh.other))

    def reduce(self, value):
        mesh, owners = self.mesh, self.owners
        chip, chips = mesh.chip, mesh.chips
        self.chip_sum[...] = value
        for shift in range(1, chips):
            owner = lax.rem(chip + shift, chips)

            @pl.when(owner < owners)
            def _():
                self.scatter(owner).start()

        @pl.when(chip < owners)
        def _():
            rest = self.got.at[pl.ds(0, chips - 1)]
            remote(rest, rest, self.sems, 2, mesh.seat(chip, mesh.core)).wait_recv()
            acc = self.chip_sum[chip]
            for shift in range(1, chips):
                acc = acc + self.got[lax.rem(chip + shift, chips)]
            self.full[mesh.core, chip] = acc
            for shift in range(1, chips):
                self.gather(lax.rem(chip + shift, chips), chip).start()
            self.gather(chip, pl.ds(0, owners - 1)).wait_recv()

        @pl.when(chip >= owners)
        def _():
            self.gather(chip, pl.ds(0, owners)).wait_recv()

        self.share().start()
        self.share().wait_recv()

    def finish(self):
        mesh, owners = self.mesh, self.owners
        chip, chips = mesh.chip, mesh.chips
        self.others().wait_send()
        for term in range(2):
            self.swap(term).wait_send()
        self.share().wait_send()

        @pl.when(chip < owners)
        def _():
            rest = self.got.at[pl.ds(0, owners - 1)]
            remote(rest, rest, self.sems, 2, mesh.seat(chip, mesh.core)).wait_send()
            rest = self.got.at[pl.ds(0, chips - 1)]
            remote(rest, rest, self.sems, 3, mesh.seat(chip, mesh.core)).wait_send()

        @pl.when(chip >= owners)
        def _():
            rest = self.got.at[pl.ds(0, owners)]
            remote(rest, rest, self.sems, 2, mesh.seat(chip, mesh.core)).wait_send()


def loads_group(lat_rows, lon_cols):
    return next(k for k in range(1, lat_rows + 1)
                if lat_rows % k == 0 and k * lon_cols % SUB == 0)


def whole(full, modes):
    blocks = [full[0, :, :, :modes].reshape(-1, modes), full[1, :, :, :modes].reshape(-1, modes)]
    return jnp.concatenate(blocks, axis=0)[:modes]


def kernel(n_lat, n_lon, total, weights, loadings, out, held, flat, scale, yh, yl, th, tl, ch, cl,
           half_gram, cubic, part1, peer1, sum1, got1, full1, rows1,
           part2, peer2, sum2, got2, full2, rows2, sems1, sems2, loads):
    lat_rows, lon_cols, modes = held.shape
    chunks, depth, _ = yh.shape
    points = lat_rows * lon_cols
    group = loads_group(lat_rows, lon_cols)
    mesh = Mesh(n_lat, n_lon)
    n, me, lat = mesh.n, mesh.me, mesh.lat
    owners = sum1.shape[0]
    reduce1 = Reduce(mesh, owners, modes, (part1, peer1, sum1, got1, full1, rows1), sems1)
    reduce2 = Reduce(mesh, owners, modes, (part2, peer2, sum2, got2, full2, rows2), sems2)

    def load(i):
        rows = pl.ds(i * group, group)
        return pltpu.make_async_copy(loadings.at[rows], held.at[rows], loads.at[i])

    for i in range(lat_rows // group):
        load(i).start()
    barrier = pltpu.get_barrier_semaphore()
    for shift in range(1, n):
        peer = lax.rem(me + shift, n)
        pl.semaphore_signal(barrier, inc=1, device_id=mesh.device(peer), device_id_type=MESH)

    flat[points:, :] = jnp.zeros((chunks * depth - points, modes), jnp.float32)
    scale[points:, :] = jnp.zeros((chunks * depth - points, scale.shape[1]), jnp.float32)
    half_gram[...] = jnp.zeros_like(half_gram)
    cubic[...] = jnp.zeros_like(cubic)

    def normalise(i, colsq):
        load(i).wait()
        ys, scales = [], []
        for k in range(group):
            j = i * group + k
            x = held[j]
            root = weights[1, lat * lat_rows + j]
            inverse = weights[2, lat * lat_rows + j]
            y = x * (root * lax.rsqrt(jnp.sum(x * x, axis=1, keepdims=True) + 1e-06))
            ys.append(y)
            scales.append(jnp.full((lon_cols, scale.shape[1]), inverse, jnp.float32))
            colsq = colsq + jnp.sum(y * y, axis=0, keepdims=True)
        rows = pl.ds(pl.multiple_of(i * group * lon_cols, SUB), group * lon_cols)
        flat[rows, :] = jnp.concatenate(ys, axis=0)
        scale[rows, :] = jnp.concatenate(scales, axis=0)
        return colsq

    none = jnp.zeros((1, modes), jnp.float32)
    colsq = lax.fori_loop(0, lat_rows // group, normalise, none)
    pl.semaphore_wait(barrier, n - 1)
    reduce1.spread(colsq)

    def cubed(value, c):
        rows = pl.ds(pl.multiple_of(c * depth, depth), depth)
        factor = scale[rows, :]
        factor = jnp.concatenate([factor] * (LANES // factor.shape[1]), axis=1)[:, :modes]
        return split(value * value * value * factor)

    unroll = next(k for k in (4, 3, 2, 1) if chunks % k == 0)

    def first(i, carry):
        grams, cubics = [], []
        for k in range(unroll):
            c = i * unroll + k
            y = flat[pl.ds(pl.multiple_of(c * depth, depth), depth), :]
            high, low = split(y)
            yh[c], yl[c] = high, low
            t_parts = split(y.T)
            th[c], tl[c] = t_parts
            grams.append(mm(t_parts[0], 0.5 * high) + mm(t_parts[0], low))
            cubics.append(mm3(t_parts, cubed(y, c)))
        half_gram[...] += sum(grams[1:], grams[0])
        cubic[...] += sum(cubics[1:], cubics[0])
        return carry

    lax.fori_loop(0, chunks // unroll, first, 0)
    reduce1.send(0, cubic[...])
    half = half_gram[...]
    gram = half + half.T
    half_gram[...] = gram
    reduce1.send(1, gram)
    cubic[...] = jnp.zeros_like(cubic)
    joined = [reduce1.joined(term) for term in range(2)]
    reduce1.reduce(joined[0] - joined[1] * (reduce1.total() / total))
    rotation = polar(whole(full1, modes))
    r_parts = split(rotation)

    turned = mm3(split(half_gram[...]), r_parts)
    reduce2.spread(jnp.sum(turned * rotation, axis=0, keepdims=True))
    reduce2.send(1, turned)

    def spin(i, carry):
        for k in range(8):
            c = i * 8 + k
            ch[c], cl[c] = cubed(mm3((yh[c], yl[c]), r_parts), c)
        return carry

    def second(i, carry):
        cubics = []
        for k in range(8):
            c = i * 8 + k
            cubics.append(mm3((th[c], tl[c]), (ch[c], cl[c])))
        cubic[...] += sum(cubics[1:], cubics[0])
        return carry

    lax.fori_loop(0, chunks // 8, spin, 0)
    lax.fori_loop(0, chunks // 8, second, 0)
    reduce2.send(0, cubic[...])
    joined = [reduce2.joined(term) for term in range(2)]
    reduce2.reduce(joined[0] - joined[1] * (reduce2.total() / total))
    out[...] = whole(full2, modes)
    reduce1.finish()
    reduce2.finish()


def turn(gradient, loadings, rotated, rotation, held, result, load, stores):
    lat_rows = held.shape[0]
    fetch = pltpu.make_async_copy(loadings, held, load)
    fetch.start()
    result[...] = polar(gradient[...])
    save = pltpu.make_async_copy(result, rotation, stores.at[0])
    save.start()
    r_parts = split(result[...])
    fetch.wait()
    unroll = next(k for k in (11, 4, 3, 2, 1) if lat_rows % k == 0)

    def step(i, carry):
        for k in range(unroll):
            j = i * unroll + k
            held[j] = mm3(split(held[j]), r_parts)
            pltpu.make_async_copy(held.at[j], rotated.at[j], stores.at[1]).start()
        return carry

    lax.fori_loop(0, lat_rows // unroll, step, 0)
    save.wait()
    pltpu.make_async_copy(held, rotated, stores.at[1]).wait()


def latitude_weight(lat_total):
    rows = np.arange(lat_total, dtype=np.float32)
    degrees = np.float32(-90.0) + (rows + np.float32(0.5)) * np.float32(180.0 / lat_total)
    return np.cos(degrees * np.float32(math.pi / 180.0)).astype(np.float32)


def shards(n_lat, n_lon, loadings):
    lat_rows, lon_cols, modes = loadings.shape
    n = n_lat * n_lon
    owners = -(-modes // (CORES * SUB))
    assert n_lat % CORES == 0 and modes % SUB == 0 and modes <= LANES
    assert 1 < owners <= n // CORES
    weights = latitude_weight(lat_rows * n_lat)
    total = float(np.sum(weights, dtype=np.float32) * np.float32(lon_cols * n_lon))
    table = jnp.asarray(np.stack([weights, np.sqrt(weights), 1.0 / weights]).astype(np.float32))
    f32, bf16 = jnp.float32, jnp.bfloat16

    bufs = [
        pltpu.VMEM((2, CORES, owners, SUB, LANES), f32),
        pltpu.VMEM((2, owners, SUB, LANES), f32),
        pltpu.VMEM((owners, SUB, LANES), f32),
        pltpu.VMEM((n // CORES, SUB, LANES), f32),
        pltpu.VMEM((CORES, owners, SUB, LANES), f32),
        pltpu.VMEM((n, 1, LANES), f32),
    ]
    points = lat_rows * lon_cols
    chunks = -(-points // DEPTH)
    group = loads_group(lat_rows, lon_cols)

    gradient = pl.pallas_call(
        functools.partial(kernel, n_lat, n_lon, total),
        out_shape=jax.ShapeDtypeStruct((modes, modes), f32),
        in_specs=[
            pl.BlockSpec(memory_space=pltpu.SMEM),
            pl.BlockSpec(memory_space=pl.ANY),
        ],
        out_specs=pl.BlockSpec(memory_space=pltpu.VMEM),
        scratch_shapes=[
            pltpu.VMEM((lat_rows, lon_cols, modes), f32),
            pltpu.VMEM((chunks * DEPTH, modes), f32),
            pltpu.VMEM((chunks * DEPTH, 128), f32),
            pltpu.VMEM((chunks, DEPTH, modes), bf16),
            pltpu.VMEM((chunks, DEPTH, modes), bf16),
            pltpu.VMEM((chunks, modes, DEPTH), bf16),
            pltpu.VMEM((chunks, modes, DEPTH), bf16),
            pltpu.VMEM((chunks, DEPTH, modes), bf16),
            pltpu.VMEM((chunks, DEPTH, modes), bf16),
            pltpu.VMEM((modes, modes), f32),
            pltpu.VMEM((modes, modes), f32),
            *bufs,
            *bufs,
            pltpu.SemaphoreType.DMA((6, 2)),
            pltpu.SemaphoreType.DMA((6, 2)),
            pltpu.SemaphoreType.DMA((lat_rows // group,)),
        ],
        compiler_params=pltpu.CompilerParams(
            collective_id=0, has_side_effects=True, vmem_limit_bytes=60 * 1024 * 1024
        ),
    )(table, loadings)
    return pl.pallas_call(
        turn,
        out_shape=(
            jax.ShapeDtypeStruct(loadings.shape, f32),
            jax.ShapeDtypeStruct((modes, modes), f32),
        ),
        in_specs=[
            pl.BlockSpec(memory_space=pltpu.VMEM),
            pl.BlockSpec(memory_space=pl.ANY),
        ],
        out_specs=(
            pl.BlockSpec(memory_space=pl.ANY),
            pl.BlockSpec(memory_space=pl.ANY),
        ),
        scratch_shapes=[
            pltpu.VMEM((lat_rows, lon_cols, modes), f32),
            pltpu.VMEM((modes, modes), f32),
            pltpu.SemaphoreType.DMA,
            pltpu.SemaphoreType.DMA((2,)),
        ],
        compiler_params=pltpu.CompilerParams(vmem_limit_bytes=60 * 1024 * 1024),
    )(gradient, loadings)


def solution(mesh):
    return jax.shard_map(
        functools.partial(shards, mesh.shape["lat"], mesh.shape["lon"]),
        mesh=mesh,
        in_specs=(P("lat", "lon", None),),
        out_specs=(P("lat", "lon", None), P()),
        check_vma=False,
    )
```
